32 devices in a mesh: dp: 2 (over x), expert: 16 (over z, y, core).
Axes of the slice: x: 2, y: 2, z: 4, core: 2. Of those that a mesh axis runs over, the one named last changes fastest.
Arguments:
- tokens: bfloat16 [4096, 2048], P(('dp', 'expert')), may hold values from -160 to 160
- router_weight: bfloat16 [2048, 16], replicated, may hold values from -0.25 to 0.25
- route_ids: int32 [4096, 2], P(('dp', 'expert')), may hold values from 0 to 15, as said below
- gate_weight: bfloat16 [16, 768, 2048], P('expert', 'dp'), may hold values from -0.125 to 0.125
- up_weight: bfloat16 [16, 768, 2048], P('expert', 'dp'), may hold values from -0.125 to 0.125
- down_weight: bfloat16 [16, 768, 2048], P('expert', 'dp'), may hold values from -0.21875 to 0.21875
Outputs:
- mixture: bfloat16 [4096, 2048], P(('dp', 'expert'))
- z_loss: float32 [], replicated
The draws below stay inside these ranges and needn't reach their ends.
Inputs may be any that keep to these rules, and one draw needn't show every extreme that they name: `route_ids`: each row names 2 different experts; among the rows of one device no expert is named more than 20 times, and one expert is named exactly 20 times by the rows of every device.
All inputs are finite; a program needn't handle non-finite values.
Results may differ from the reference program's by a relative error of at most 0.0057.
Values may be sent and summed in bfloat16 or wider, within the bound.
No kernel may reach another device: no remote copies, remote signals or barrier semaphores. Data moves between devices by JAX's collectives and lax.ppermute only.
A program may use at most 64 MiB of HBM per device.

```python
import math
import jax
import jax.numpy as jnp
from jax import lax

D = 2048
FF = 768
EXP_DEV = 1
TOPK = 2
TOK_DEV = 128
EXPERTS = 16
CAP = 20
TOKENS = 4096


def router_table(key):
    base_key = jax.random.fold_in(key, 7)
    bound_value = math.sqrt(3.0 / D)
    values = jax.random.uniform(base_key, (D, EXPERTS), jnp.float32, -bound_value, bound_value)
    return values.astype(jnp.bfloat16).astype(jnp.float32)


def expert_order(subkey):
    return jax.random.permutation(subkey, EXPERTS)


def token_order(subkey):
    return jax.random.permutation(subkey, TOK_DEV)


def route_table(key):
    blocks = TOKENS // TOK_DEV
    slots_dev = TOK_DEV * TOPK
    base_count = slots_dev // EXPERTS
    spare = CAP - base_count
    half_count = EXPERTS // 2
    key_pairs, key_moves, key_order, key_rows = jax.random.split(jax.random.fold_in(key, 3), 4)
    pairing = jax.random.permutation(key_pairs, EXPERTS)
    moves = jax.random.randint(key_moves, (blocks, half_count), 0, spare + 1)
    moves = moves.at[:, 0].set(spare)
    paired = jnp.stack([base_count + moves, base_count - moves], axis=2).reshape(blocks, EXPERTS)
    counts = jnp.zeros((blocks, EXPERTS), jnp.int32).at[:, pairing].set(paired.astype(jnp.int32))
    orders = jax.vmap(expert_order)(jax.random.split(key_order, blocks))
    ordered_counts = jnp.take_along_axis(counts, orders, axis=1)
    bounds = jnp.cumsum(ordered_counts, axis=1)
    slot_pos = jnp.arange(slots_dev, dtype=jnp.int32)
    run_index = jnp.sum((bounds[:, None, :] <= slot_pos[None, :, None]).astype(jnp.int32), axis=2)
    expert_at = jnp.take_along_axis(orders, run_index, axis=1)
    route_grid = expert_at.reshape(blocks, TOPK, TOK_DEV).transpose(0, 2, 1)
    shuffles = jax.vmap(token_order)(jax.random.split(key_rows, blocks))
    route_grid = jnp.take_along_axis(route_grid, shuffles[:, :, None], axis=1)
    return route_grid.reshape(TOKENS, TOPK).astype(jnp.int32)


def close_gaps(values, router, routes, target_key):
    logits = jnp.dot(values, router, precision=lax.Precision.HIGHEST)
    expert_ids = jnp.arange(EXPERTS, dtype=jnp.int32)[None, :]
    first_hot = (routes[:, 0:1] == expert_ids).astype(jnp.float32)
    second_hot = (routes[:, 1:2] == expert_ids).astype(jnp.float32)
    diff_hot = first_hot - second_hot
    current_gap = jnp.sum(logits * diff_hot, axis=1)
    gram = jnp.dot(router.T, router, precision=lax.Precision.HIGHEST)
    diff_norm = jnp.sum(jnp.dot(diff_hot, gram, precision=lax.Precision.HIGHEST) * diff_hot, axis=1)
    target_gap = jax.random.uniform(target_key, (TOKENS,), jnp.float32, -2.5, 2.5)
    coefficient = (target_gap - current_gap) / diff_norm
    shift_rows = jnp.dot(coefficient[:, None] * diff_hot, router.T, precision=lax.Precision.HIGHEST)
    return values + shift_rows


def draw_router_weight(key, part):
    return router_table(key).astype(jnp.bfloat16)


def draw_route_ids(key, part):
    return route_table(key)


def draw_tokens(key, part):
    blocks = TOKENS // TOK_DEV
    groups = EXPERTS // EXP_DEV
    lanes = blocks // groups
    device = jnp.arange(TOKENS) // TOK_DEV
    along = (device % groups).astype(jnp.float32) / max(groups - 1, 1)
    across = (device // groups).astype(jnp.float32) / max(lanes - 1, 1)
    ramp_scale = (0.5 + 2.3 * along) * (1.0 + across)
    key_noise, key_scale = jax.random.split(jax.random.fold_in(key, 5), 2)
    key_target = jax.random.fold_in(key, 11)
    router = router_table(key)
    routes = route_table(key)
    spread = jnp.exp(jax.random.uniform(key_scale, (TOKENS,), jnp.float32, math.log(0.6), math.log(1.6)))
    noise_part = jax.random.normal(key_noise, (TOKENS, D), jnp.float32)
    values = noise_part * (ramp_scale * spread)[:, None]
    values = close_gaps(values, router, routes, key_target)
    return jnp.clip(values, -160.0, 160.0).astype(jnp.bfloat16)


def block_scale(key, shape, shards, smallest, top_value):
    loudness = 1.0
    for axis_at, shards_of in shards:
        heights = jax.random.uniform(jax.random.fold_in(jax.random.fold_in(key, 6), axis_at), (shards_of,), jnp.float32, smallest / len(shards), top_value / len(shards))
        loudness = loudness * jnp.repeat(jnp.exp(heights), shape[axis_at] // shards_of).reshape((-1,) + (1,) * (len(shape) - 1 - axis_at))
    return loudness


def scatter_about(stream_key, dims, scale, reach, cuts=(), kind=jnp.bfloat16):
    entries = jax.random.normal(stream_key, dims, jnp.float32) * scale
    if len(cuts) > 0:
        entries = block_scale(stream_key, dims, cuts, -0.22, 0.18) * entries
    return jnp.clip(entries, min=-reach, max=reach).astype(kind)


def setup_inputs(seed: int = 0) -> dict:
    keys = jax.random.split(jax.random.key(seed), 7)
    tokens = draw_tokens(jax.random.fold_in(keys[6], 71), 0)
    router_weight = draw_router_weight(jax.random.fold_in(keys[6], 71), 0)
    route_ids = draw_route_ids(jax.random.fold_in(keys[6], 71), 0)
    gate_weight = scatter_about(keys[3], (EXPERTS, FF, D), D ** -0.5, 0.125, ((0, 16), (1, 2)))
    up_weight = scatter_about(keys[4], (EXPERTS, FF, D), D ** -0.5, 0.125, ((0, 16), (1, 2)))
    down_weight = scatter_about(keys[5], (EXPERTS, FF, D), FF ** -0.5, 0.21875, ((0, 16), (1, 2)))
    return {"tokens": tokens, "router_weight": router_weight, "route_ids": route_ids, "gate_weight": gate_weight, "up_weight": up_weight, "down_weight": down_weight}


def block_tables(ids_block, weights_block):
    flat_ids = ids_block.reshape(-1)
    onehot = (flat_ids[:, None] == jnp.arange(EXPERTS, dtype=jnp.int32)[None, :]).astype(jnp.int32)
    before = jnp.cumsum(onehot, axis=0) - onehot
    position = jnp.sum(before * onehot, axis=1)
    slots = flat_ids * CAP + position
    slot_match = slots[None, :] == jnp.arange(EXPERTS * CAP, dtype=jnp.int32)[:, None]
    token_of = jnp.arange(TOK_DEV * TOPK, dtype=jnp.int32) // TOPK
    source_row = jnp.sum(jnp.where(slot_match, token_of[None, :], 0), axis=1).astype(jnp.int32)
    filled = jnp.any(slot_match, axis=1)
    flat_weights = weights_block.reshape(-1)
    slot_weight = jnp.sum(jnp.where(slot_match, flat_weights[None, :], jnp.zeros((), flat_weights.dtype)), axis=1)
    return source_row, filled, slot_weight


def tables_of(block_pair):
    return block_tables(block_pair[0], block_pair[1])


def reference(tokens, router_weight, route_ids, gate_weight, up_weight, down_weight):
    logits = jnp.dot(tokens, router_weight, preferred_element_type=jnp.float32)
    log_total = jax.nn.logsumexp(logits, axis=1)
    z_loss = jnp.mean(log_total * log_total)
    chosen = jnp.take_along_axis(logits, route_ids, axis=1)
    route_weight = jax.nn.softmax(chosen, axis=1)
    blocks = TOKENS // TOK_DEV
    source_row, filled, slot_weight = lax.map(tables_of, (route_ids.reshape(blocks, TOK_DEV, TOPK), route_weight.reshape(blocks, TOK_DEV, TOPK)))
    offsets = (jnp.arange(blocks, dtype=jnp.int32) * TOK_DEV)[:, None]
    global_row = (source_row + offsets).astype(jnp.int32)

    def by_expert(table):
        return table.reshape(blocks, EXPERTS, CAP).transpose(1, 0, 2).reshape(EXPERTS, blocks * CAP)

    def expert_step(accumulated, inputs):
        gate_one, up_one, down_one, rows_one, filled_one, weight_one = inputs
        expert_rows = jnp.where(filled_one[:, None], tokens[rows_one], jnp.zeros((), tokens.dtype))
        rows_wide = expert_rows.astype(jnp.float32)
        gate_val = jnp.dot(rows_wide, gate_one.astype(jnp.float32).T, preferred_element_type=jnp.float32)
        up_val = jnp.dot(rows_wide, up_one.astype(jnp.float32).T, preferred_element_type=jnp.float32)
        hidden = (jax.nn.silu(gate_val) * up_val).astype(jnp.bfloat16)
        expert_out = jnp.dot(hidden.astype(jnp.float32), down_one.astype(jnp.float32), preferred_element_type=jnp.float32).astype(jnp.bfloat16)
        accumulated = accumulated.at[rows_one].add(weight_one[:, None] * expert_out.astype(jnp.float32))
        return accumulated, None

    initial = jnp.zeros((TOKENS, D), jnp.float32)
    accumulated, unused = lax.scan(expert_step, initial, (gate_weight, up_weight, down_weight, by_expert(global_row), by_expert(filled), by_expert(slot_weight)))
    return accumulated.astype(jnp.bfloat16), z_loss
```

```python
import jax
import jax.numpy as jnp
from jax import lax
from jax.sharding import PartitionSpec as P


def column_parts(capacity):
    parts = 1
    while (parts * capacity) % 8:
        parts *= 2
    return parts


def swap_dp(value):
    size = lax.axis_size("dp")
    return [lax.ppermute(value, "dp", [(s, (s + k) % size) for s in range(size)]) for k in range(1, size)]


def return_dp(values):
    size = lax.axis_size("dp")
    return [
        lax.ppermute(v, "dp", [(s, (s - k) % size) for s in range(size)])
        for k, v in enumerate(values, 1)
    ]


def pack(rows, blocks, parts):
    capacity = rows.shape[0] // blocks
    width = rows.shape[1] // parts
    return (
        rows.reshape(blocks, capacity, parts, width)
        .transpose(0, 2, 1, 3)
        .reshape(blocks, parts * capacity, width)
    )


def unpack(packed, parts):
    blocks, tall, width = packed.shape
    capacity = tall // parts
    return (
        packed.reshape(blocks, parts, capacity, width)
        .transpose(0, 2, 1, 3)
        .reshape(blocks * capacity, parts * width)
    )


def on_device(tokens, router_weight, route_ids, gate_weight, up_weight, down_weight):
    rows_here, model_width = tokens.shape
    top_count = route_ids.shape[1]
    experts = router_weight.shape[1]
    owners = lax.axis_size("expert")
    capacity = 5 * rows_here * top_count // (4 * experts)
    parts = column_parts(capacity)
    tall = parts * capacity
    width = model_width // parts
    gate, up, down = gate_weight[0], up_weight[0], down_weight[0]
    down_other = swap_dp(down)

    expert_at = jnp.arange(experts, dtype=jnp.int32)[:, None]
    ids_t = route_ids.T
    routed = ids_t[0][None, :] == expert_at
    for k in range(1, top_count):
        routed = routed | (ids_t[k][None, :] == expert_at)
    earlier = jnp.arange(rows_here)[:, None] < jnp.arange(rows_here)[None, :]
    before = jnp.dot(
        routed.astype(jnp.bfloat16), earlier.astype(jnp.bfloat16), preferred_element_type=jnp.float32
    )
    position = jnp.where(routed, before, -1.0)
    position_wide = jnp.tile(position, (1, parts))
    tall_at = jnp.arange(tall, dtype=jnp.int32)[None, :, None]
    wide_at = jnp.arange(parts * rows_here, dtype=jnp.int32)[None, None, :]
    match = (position_wide[:, None, :] == (tall_at % capacity).astype(jnp.float32)) & (
        tall_at // capacity == wide_at // rows_here
    )
    stacked = jnp.concatenate(
        [tokens[:, p * width : (p + 1) * width] for p in range(parts)], axis=0
    )
    dispatch = jnp.dot(
        match.astype(jnp.bfloat16).reshape(experts * tall, parts * rows_here),
        stacked,
        preferred_element_type=jnp.float32,
    ).astype(jnp.bfloat16)
    received = lax.all_to_all(
        dispatch.reshape(experts, tall, width), "expert", split_axis=0, concat_axis=0, tiled=True
    )
    others = swap_dp(received)

    tokens_late, router_late, received = lax.optimization_barrier((tokens, router_weight, received))
    logits = lax.dot_general(
        router_late, tokens_late, (((0,), (1,)), ((), ())), preferred_element_type=jnp.float32
    )
    log_total = jax.nn.logsumexp(logits, axis=0)
    local_sum = jnp.sum(log_total * log_total)
    total_sum = lax.psum(local_sum, ("dp", "expert"))
    token_total = rows_here * lax.axis_size("dp") * owners
    z_loss = total_sum / jnp.float32(token_total)
    top_logit = jnp.max(jnp.where(routed, logits, -jnp.inf), axis=0, keepdims=True)
    route_exp = jnp.where(routed, jnp.exp(logits - top_logit), 0.0)
    route_weight = route_exp / jnp.sum(route_exp, axis=0, keepdims=True)
    weight_high = lax.reduce_precision(route_weight, 8, 7)
    weight_low = route_weight - weight_high

    def spread(values):
        wide = jnp.tile(values, (1, parts))[:, None, :]
        return jnp.where(match, wide, 0.0).astype(jnp.bfloat16).reshape(experts * tall, parts * rows_here)

    combine = jnp.concatenate([spread(weight_high), spread(weight_low)], axis=1)

    def half_hidden(packed):
        rows = unpack(packed, parts)
        contract = (((1,), (1,)), ((), ()))
        gate_val = lax.dot_general(rows, gate, contract, preferred_element_type=jnp.float32)
        up_val = lax.dot_general(rows, up, contract, preferred_element_type=jnp.float32)
        return (jax.nn.silu(gate_val) * up_val).astype(jnp.bfloat16)

    own_hidden = half_hidden(received)
    z_loss, others, combine, own_hidden = lax.optimization_barrier((z_loss, others, combine, own_hidden))
    back = return_dp([half_hidden(o) for o in others])
    size = lax.axis_size("dp")
    summed = jnp.dot(own_hidden, down, preferred_element_type=jnp.float32)
    for k in range(1, size):
        summed = summed + jnp.dot(back[k - 1], down_other[size - k - 1], preferred_element_type=jnp.float32)
    outgoing = pack(summed.astype(jnp.bfloat16), owners, parts)
    returned = lax.all_to_all(outgoing, "expert", split_axis=0, concat_axis=0, tiled=True)
    mixed = lax.dot_general(
        combine,
        returned.reshape(experts * tall, width),
        (((0,), (0,)), ((), ())),
        preferred_element_type=jnp.float32,
    )
    mixed = jnp.sum(mixed.reshape(2, parts, rows_here, width), axis=0).astype(jnp.bfloat16)
    return jnp.concatenate([mixed[p] for p in range(parts)], axis=1), z_loss


def solution(mesh):
    in_specs = (
        P(("dp", "expert"), None),
        P(),
        P(("dp", "expert"), None),
        P("expert", "dp", None),
        P("expert", "dp", None),
        P("expert", "dp", None),
    )
    out_specs = (P(("dp", "expert"), None), P())
    return jax.shard_map(
        on_device, mesh=mesh, in_specs=in_specs, out_specs=out_specs, check_vma=False
    )
```

```python
import jax
import jax.numpy as jnp
from jax import lax
from jax.sharding import PartitionSpec as P


def column_parts(capacity):
    parts = 1
    while (parts * capacity) % 8:
        parts *= 2
    return parts


def swap_dp(value):
    size = lax.axis_size("dp")
    return [lax.ppermute(value, "dp", [(s, (s + k) % size) for s in range(size)]) for k in range(1, size)]


def return_dp(values):
    size = lax.axis_size("dp")
    return [
        lax.ppermute(v, "dp", [(s, (s - k) % size) for s in range(size)])
        for k, v in enumerate(values, 1)
    ]


def regroup(blocks, parts, capacity, back):
    total = blocks * parts * capacity
    packed_at = jnp.arange(total, dtype=jnp.int32)
    block = packed_at // (parts * capacity)
    part = packed_at // capacity % parts
    target = (part * blocks + block) * capacity + packed_at % capacity
    flat_at = jnp.arange(total, dtype=jnp.int32)
    hot = flat_at[None, :] == target[:, None] if back else flat_at[:, None] == target[None, :]
    return hot.astype(jnp.bfloat16)


def exact(hot, rows):
    return jnp.dot(hot, rows, preferred_element_type=jnp.float32).astype(jnp.bfloat16)


def sum_over(value, axis):
    size = lax.axis_size(axis)
    if size & (size - 1):
        return lax.psum(value, axis)
    step = 1
    while step < size:
        value = value + lax.ppermute(value, axis, [(s, s ^ step) for s in range(size)])
        step *= 2
    return value


def on_device(tokens, router_weight, route_ids, gate_weight, up_weight, down_weight):
    rows_here, model_width = tokens.shape
    top_count = route_ids.shape[1]
    experts = router_weight.shape[1]
    owners = lax.axis_size("expert")
    capacity = 5 * rows_here * top_count // (4 * experts)
    parts = column_parts(capacity)
    tall = parts * capacity
    width = model_width // parts
    gate, up, down = gate_weight[0], up_weight[0], down_weight[0]
    down_other = swap_dp(down)

    expert_at = jnp.arange(experts, dtype=jnp.int32)[:, None]
    ids_t = route_ids.T
    routed = ids_t[0][None, :] == expert_at
    for k in range(1, top_count):
        routed = routed | (ids_t[k][None, :] == expert_at)
    earlier = jnp.arange(rows_here)[:, None] < jnp.arange(rows_here)[None, :]
    before = jnp.dot(
        routed.astype(jnp.bfloat16), earlier.astype(jnp.bfloat16), preferred_element_type=jnp.float32
    )
    position = jnp.where(routed, before, -1.0)
    position_wide = jnp.tile(position, (1, parts))
    tall_at = jnp.arange(tall, dtype=jnp.int32)[None, :, None]
    wide_at = jnp.arange(parts * rows_here, dtype=jnp.int32)[None, None, :]
    match = (position_wide[:, None, :] == (tall_at % capacity).astype(jnp.float32)) & (
        tall_at // capacity == wide_at // rows_here
    )
    stacked = jnp.concatenate(
        [tokens[:, p * width : (p + 1) * width] for p in range(parts)], axis=0
    )
    dispatch = jnp.dot(
        match.astype(jnp.bfloat16).reshape(experts * tall, parts * rows_here),
        stacked,
        preferred_element_type=jnp.float32,
    ).astype(jnp.bfloat16)
    received = lax.all_to_all(
        dispatch.reshape(experts, tall, width), "expert", split_axis=0, concat_axis=0, tiled=True
    )
    others = swap_dp(received)

    tokens_late, router_late, received = lax.optimization_barrier((tokens, router_weight, received))
    logits = lax.dot_general(
        router_late, tokens_late, (((0,), (1,)), ((), ())), preferred_element_type=jnp.float32
    )
    log_total = jax.nn.logsumexp(logits, axis=0)
    local_sum = jnp.sum(log_total * log_total)
    group_sum = sum_over(jnp.full((8, 128), local_sum), "expert")
    top_logit = jnp.max(jnp.where(routed, logits, -jnp.inf), axis=0, keepdims=True)
    route_exp = jnp.where(routed, jnp.exp(logits - top_logit), 0.0)
    route_weight = route_exp / jnp.sum(route_exp, axis=0, keepdims=True)
    weight_high = lax.reduce_precision(route_weight, 8, 7)
    weight_low = route_weight - weight_high

    def spread(values):
        wide = jnp.tile(values, (1, parts))[:, None, :]
        return jnp.where(match, wide, 0.0).astype(jnp.bfloat16).reshape(experts * tall, parts * rows_here)

    combine = jnp.concatenate([spread(weight_high), spread(weight_low)], axis=1)

    to_parts = regroup(owners, parts, capacity, False)
    to_blocks = regroup(owners, parts, capacity, True)
    rows_all = owners * capacity

    def half_hidden(packed):
        stack = exact(to_parts, packed.reshape(owners * tall, width))
        rows = jnp.concatenate(
            [stack[p * rows_all : (p + 1) * rows_all] for p in range(parts)], axis=1
        )
        contract = (((1,), (1,)), ((), ()))
        gate_val = lax.dot_general(rows, gate, contract, preferred_element_type=jnp.float32)
        up_val = lax.dot_general(rows, up, contract, preferred_element_type=jnp.float32)
        return (jax.nn.silu(gate_val) * up_val).astype(jnp.bfloat16)

    own_hidden = half_hidden(received)
    group_sum, others, combine, own_hidden, to_blocks = lax.optimization_barrier(
        (group_sum, others, combine, own_hidden, to_blocks)
    )
    back = return_dp([half_hidden(o) for o in others])
    total_sum = sum_over(group_sum, "dp")
    total_sum, back = lax.optimization_barrier((total_sum, back))
    token_total = rows_here * lax.axis_size("dp") * owners
    z_loss = total_sum[0, 0] / jnp.float32(token_total)
    size = lax.axis_size("dp")
    pieces = []
    for p in range(parts):
        cols = slice(p * width, (p + 1) * width)
        summed = jnp.dot(own_hidden, down[:, cols], preferred_element_type=jnp.float32)
        for k in range(1, size):
            summed = summed + jnp.dot(
                back[k - 1], down_other[size - k - 1][:, cols], preferred_element_type=jnp.float32
            )
        pieces.append(summed.astype(jnp.bfloat16))
    outgoing = exact(to_blocks, jnp.concatenate(pieces, axis=0)).reshape(experts, tall, width)
    returned = lax.all_to_all(outgoing, "expert", split_axis=0, concat_axis=0, tiled=True)
    mixed = lax.dot_general(
        combine,
        returned.reshape(experts * tall, width),
        (((0,), (0,)), ((), ())),
        preferred_element_type=jnp.float32,
    )
    mixed = jnp.sum(mixed.reshape(2, parts, rows_here, width), axis=0).astype(jnp.bfloat16)
    return jnp.concatenate([mixed[p] for p in range(parts)], axis=1), z_loss


def solution(mesh):
    in_specs = (
        P(("dp", "expert"), None),
        P(),
        P(("dp", "expert"), None),
        P("expert", "dp", None),
        P("expert", "dp", None),
        P("expert", "dp", None),
    )
    out_specs = (P(("dp", "expert"), None), P())
    return jax.shard_map(
        on_device, mesh=mesh, in_specs=in_specs, out_specs=out_specs, check_vma=False
    )
```

```python
import jax
import jax.numpy as jnp
from jax import lax
from jax.sharding import PartitionSpec as P


def column_parts(capacity):
    parts = 1
    while (parts * capacity) % 8:
        parts *= 2
    return parts


def toward(size, step):
    if size & (size - 1):
        return [(s, (s + step) % size) for s in range(size)]
    return [(s, s ^ step) for s in range(size)]


def send(value, axis, step, back=False):
    pairs = toward(lax.axis_size(axis), step)
    return lax.ppermute(value, axis, [(t, s) for s, t in pairs] if back else pairs)


def regroup(blocks, parts, capacity, back):
    total = blocks * parts * capacity
    packed_at = jnp.arange(total, dtype=jnp.int32)
    block = packed_at // (parts * capacity)
    part = packed_at // capacity % parts
    target = (part * blocks + block) * capacity + packed_at % capacity
    flat_at = jnp.arange(total, dtype=jnp.int32)
    hot = flat_at[None, :] == target[:, None] if back else flat_at[:, None] == target[None, :]
    return hot.astype(jnp.bfloat16)


def exact(hot, rows):
    return jnp.dot(hot, rows, preferred_element_type=jnp.float32).astype(jnp.bfloat16)


def sum_over(value, axis):
    size = lax.axis_size(axis)
    if size & (size - 1):
        return lax.psum(value, axis)
    step = 1
    while step < size:
        value = value + lax.ppermute(value, axis, [(s, s ^ step) for s in range(size)])
        step *= 2
    return value


def on_device(tokens, router_weight, route_ids, gate_weight, up_weight, down_weight):
    rows_here, model_width = tokens.shape
    top_count = route_ids.shape[1]
    experts = router_weight.shape[1]
    owners = lax.axis_size("expert")
    replicas = lax.axis_size("dp")
    capacity = 5 * rows_here * top_count // (4 * experts)
    parts = column_parts(capacity)
    tall = parts * capacity
    width = model_width // parts
    gate, up, down = gate_weight[0], up_weight[0], down_weight[0]

    here = lax.axis_index("expert")
    steps = jnp.arange(owners, dtype=jnp.int32)
    reached = (here + steps) % owners if owners & (owners - 1) else here ^ steps
    expert_at = reached[:, None]
    ids_t = route_ids.T
    routed_by = [ids_t[k][None, :] == expert_at for k in range(top_count)]
    routed = routed_by[0]
    for k in range(1, top_count):
        routed = routed | routed_by[k]
    earlier = jnp.arange(rows_here)[:, None] < jnp.arange(rows_here)[None, :]
    before = jnp.dot(
        routed.astype(jnp.bfloat16), earlier.astype(jnp.bfloat16), preferred_element_type=jnp.float32
    )
    position = jnp.where(routed, before, -1.0)
    position_wide = jnp.tile(position, (1, parts))
    tall_at = jnp.arange(tall, dtype=jnp.int32)[None, :, None]
    wide_at = jnp.arange(parts * rows_here, dtype=jnp.int32)[None, None, :]
    match = (position_wide[:, None, :] == (tall_at % capacity).astype(jnp.float32)) & (
        tall_at // capacity == wide_at // rows_here
    )
    stacked = jnp.concatenate(
        [tokens[:, p * width : (p + 1) * width] for p in range(parts)], axis=0
    )
    dispatch = exact(match.astype(jnp.bfloat16).reshape(experts * tall, parts * rows_here), stacked)
    dispatch = dispatch.reshape(owners, tall, width)

    groups = 4 if owners % 4 == 0 else 1
    per = owners // groups
    arrived = [
        dispatch[o] if o == 0 else send(dispatch[o], "expert", o) for o in range(owners)
    ]

    to_parts = regroup(replicas * per, parts, capacity, False)
    to_blocks = regroup(per, parts, capacity, True)
    rows_all = replicas * per * capacity
    rows_one = per * capacity
    contract = (((1,), (1,)), ((), ()))
    mine = [jnp.concatenate(arrived[g * per : (g + 1) * per], axis=0) for g in range(groups)]
    partial = []
    theirs = [[send(m, "dp", k) for k in range(1, replicas)] for m in mine[:2]]
    for g in range(groups):
        stack = exact(to_parts, jnp.concatenate([mine[g]] + theirs[g], axis=0))
        rows = jnp.concatenate(
            [stack[p * rows_all : (p + 1) * rows_all] for p in range(parts)], axis=1
        )
        gate_val = lax.dot_general(rows, gate, contract, preferred_element_type=jnp.float32)
        up_val = lax.dot_general(rows, up, contract, preferred_element_type=jnp.float32)
        hidden = (jax.nn.silu(gate_val) * up_val).astype(jnp.bfloat16)
        own = jnp.dot(hidden[:rows_one], down, preferred_element_type=jnp.float32)
        other = exact(hidden[rows_one:], down)
        back = [
            send(other[(k - 1) * rows_one : k * rows_one], "dp", k, True) for k in range(1, replicas)
        ]
        partial.append((own, back))
        if g + 2 < groups:
            mine[g + 2], other = lax.optimization_barrier((mine[g + 2], other))
            theirs.append([send(mine[g + 2], "dp", k) for k in range(1, replicas)])

    returned = []
    for g in range(groups):
        own, back = partial[g]
        summed = own
        for piece in back:
            summed = summed + piece.astype(jnp.float32)
        summed = summed.astype(jnp.bfloat16)
        flat = jnp.concatenate([summed[:, p * width : (p + 1) * width] for p in range(parts)], axis=0)
        outgoing = exact(to_blocks, flat).reshape(per, tall, width)
        for i in range(per):
            o = g * per + i
            returned.append(outgoing[i] if o == 0 else send(outgoing[i], "expert", o, True))

    tokens_late, router_late, unused = lax.optimization_barrier((tokens, router_weight, mine[-1]))
    logits = lax.dot_general(
        router_late, tokens_late, (((0,), (1,)), ((), ())), preferred_element_type=jnp.float32
    )
    log_total = jax.nn.logsumexp(logits, axis=0)
    local_sum = jnp.sum(log_total * log_total)
    group_sum = sum_over(jnp.full((8, 128), local_sum), "expert")
    group_sum, unused = lax.optimization_barrier((group_sum, other))
    total_sum = sum_over(group_sum, "dp")
    z_loss = total_sum[0, 0] / jnp.float32(rows_here * replicas * owners)
    true_at = jnp.arange(experts, dtype=jnp.int32)[:, None]
    chosen = jnp.stack(
        [jnp.sum(jnp.where(ids_t[k][None, :] == true_at, logits, 0.0), axis=0) for k in range(top_count)]
    )
    choice_weight = jax.nn.softmax(chosen, axis=0)
    route_weight = jnp.zeros((owners, rows_here), jnp.float32)
    for k in range(top_count):
        route_weight = jnp.where(routed_by[k], choice_weight[k][None, :], route_weight)
    weight_high = lax.reduce_precision(route_weight, 8, 7)
    weight_low = route_weight - weight_high

    def spread(values):
        wide = jnp.tile(values, (1, parts))[:, None, :]
        return jnp.where(match, wide, 0.0).astype(jnp.bfloat16).reshape(experts * tall, parts * rows_here)

    combine = jnp.concatenate([spread(weight_high), spread(weight_low)], axis=1)
    mixed = lax.dot_general(
        combine,
        jnp.concatenate(returned, axis=0),
        (((0,), (0,)), ((), ())),
        preferred_element_type=jnp.float32,
    )
    mixed = jnp.sum(mixed.reshape(2, parts, rows_here, width), axis=0).astype(jnp.bfloat16)
    return jnp.concatenate([mixed[p] for p in range(parts)], axis=1), z_loss


def solution(mesh):
    in_specs = (
        P(("dp", "expert"), None),
        P(),
        P(("dp", "expert"), None),
        P("expert", "dp", None),
        P("expert", "dp", None),
        P("expert", "dp", None),
    )
    out_specs = (P(("dp", "expert"), None), P())
    return jax.shard_map(
        on_device, mesh=mesh, in_specs=in_specs, out_specs=out_specs, check_vma=False
    )
```

```python
import jax
import jax.numpy as jnp
from jax import lax
from jax.sharding import PartitionSpec as P


def column_parts(capacity):
    parts = 1
    while (parts * capacity) % 8:
        parts *= 2
    return parts


def toward(size, step):
    if size & (size - 1):
        return [(s, (s + step) % size) for s in range(size)]
    return [(s, s ^ step) for s in range(size)]


def send(value, axis, step, back=False):
    pairs = toward(lax.axis_size(axis), step)
    return lax.ppermute(value, axis, [(t, s) for s, t in pairs] if back else pairs)


def regroup(blocks, parts, capacity, back):
    total = blocks * parts * capacity
    packed_at = jnp.arange(total, dtype=jnp.int32)
    block = packed_at // (parts * capacity)
    part = packed_at // capacity % parts
    target = (part * blocks + block) * capacity + packed_at % capacity
    flat_at = jnp.arange(total, dtype=jnp.int32)
    hot = flat_at[None, :] == target[:, None] if back else flat_at[:, None] == target[None, :]
    return hot.astype(jnp.bfloat16)


def exact(hot, rows):
    return jnp.dot(hot, rows, preferred_element_type=jnp.float32).astype(jnp.bfloat16)


def sum_over(value, axis):
    size = lax.axis_size(axis)
    if size & (size - 1):
        return lax.psum(value, axis)
    step = 1
    while step < size:
        value = value + lax.ppermute(value, axis, [(s, s ^ step) for s in range(size)])
        step *= 2
    return value


def on_device(tokens, router_weight, route_ids, gate_weight, up_weight, down_weight):
    rows_here, model_width = tokens.shape
    top_count = route_ids.shape[1]
    experts = router_weight.shape[1]
    owners = lax.axis_size("expert")
    replicas = lax.axis_size("dp")
    capacity = 5 * rows_here * top_count // (4 * experts)
    parts = column_parts(capacity)
    tall = parts * capacity
    width = model_width // parts
    gate, up, down = gate_weight[0], up_weight[0], down_weight[0]

    here = lax.axis_index("expert")
    steps = jnp.arange(owners, dtype=jnp.int32)
    reached = (here + steps) % owners if owners & (owners - 1) else here ^ steps
    expert_at = reached[:, None]
    ids_t = route_ids.T
    routed_by = [ids_t[k][None, :] == expert_at for k in range(top_count)]
    routed = routed_by[0]
    for k in range(1, top_count):
        routed = routed | routed_by[k]
    earlier = jnp.arange(rows_here)[:, None] < jnp.arange(rows_here)[None, :]
    before = jnp.dot(
        routed.astype(jnp.bfloat16), earlier.astype(jnp.bfloat16), preferred_element_type=jnp.float32
    )
    position = jnp.where(routed, before, -1.0)
    position_wide = jnp.tile(position, (1, parts))
    tall_at = jnp.arange(tall, dtype=jnp.int32)[None, :, None]
    wide_at = jnp.arange(parts * rows_here, dtype=jnp.int32)[None, None, :]
    match = (position_wide[:, None, :] == (tall_at % capacity).astype(jnp.float32)) & (
        tall_at // capacity == wide_at // rows_here
    )
    stacked = jnp.concatenate(
        [tokens[:, p * width : (p + 1) * width] for p in range(parts)], axis=0
    )
    dispatch = exact(match.astype(jnp.bfloat16).reshape(experts * tall, parts * rows_here), stacked)
    dispatch = dispatch.reshape(owners, tall, width)

    groups = 4 if owners % 4 == 0 else 1
    per = owners // groups
    arrived = [
        dispatch[o] if o == 0 else send(dispatch[o], "expert", o) for o in range(owners)
    ]

    to_parts = regroup(replicas * per, parts, capacity, False)
    to_blocks = regroup(per, parts, capacity, True)
    rows_all = replicas * per * capacity
    rows_one = per * capacity
    contract = (((1,), (1,)), ((), ()))
    mine = [jnp.concatenate(arrived[g * per : (g + 1) * per], axis=0) for g in range(groups)]
    partial = []
    theirs = [[send(m, "dp", k) for k in range(1, replicas)] for m in mine[:2]]
    for g in range(groups):
        stack = exact(to_parts, jnp.concatenate([mine[g]] + theirs[g], axis=0))
        rows = jnp.concatenate(
            [stack[p * rows_all : (p + 1) * rows_all] for p in range(parts)], axis=1
        )
        gate_val = lax.dot_general(rows, gate, contract, preferred_element_type=jnp.float32)
        up_val = lax.dot_general(rows, up, contract, preferred_element_type=jnp.float32)
        hidden = (jax.nn.silu(gate_val) * up_val).astype(jnp.bfloat16)
        own = jnp.dot(hidden[:rows_one], down, preferred_element_type=jnp.float32)
        other = exact(hidden[rows_one:], down)
        back = [
            send(other[(k - 1) * rows_one : k * rows_one], "dp", k, True) for k in range(1, replicas)
        ]
        partial.append((own, back))
        if g + 2 < groups:
            mine[g + 2], other = lax.optimization_barrier((mine[g + 2], other))
            theirs.append([send(mine[g + 2], "dp", k) for k in range(1, replicas)])

    returned = []
    for g in range(groups):
        own, back = partial[g]
        summed = own
        for piece in back:
            summed = summed + piece.astype(jnp.float32)
        summed = summed.astype(jnp.bfloat16)
        flat = jnp.concatenate([summed[:, p * width : (p + 1) * width] for p in range(parts)], axis=0)
        outgoing = exact(to_blocks, flat).reshape(per, tall, width)
        for i in range(per):
            o = g * per + i
            returned.append(outgoing[i] if o == 0 else send(outgoing[i], "expert", o, True))

    tokens_late, router_late, unused = lax.optimization_barrier((tokens, router_weight, outgoing))
    logits = lax.dot_general(
        router_late, tokens_late, (((0,), (1,)), ((), ())), preferred_element_type=jnp.float32
    )
    log_total = jax.nn.logsumexp(logits, axis=0)
    local_sum = jnp.sum(log_total * log_total)
    group_sum = sum_over(jnp.full((8, 128), local_sum), "expert")
    group_sum, unused = lax.optimization_barrier((group_sum, other))
    total_sum = sum_over(group_sum, "dp")
    z_loss = total_sum[0, 0] / jnp.float32(rows_here * replicas * owners)
    true_at = jnp.arange(experts, dtype=jnp.int32)[:, None]
    chosen = jnp.stack(
        [jnp.sum(jnp.where(ids_t[k][None, :] == true_at, logits, 0.0), axis=0) for k in range(top_count)]
    )
    choice_weight = jax.nn.softmax(chosen, axis=0)
    route_weight = jnp.zeros((owners, rows_here), jnp.float32)
    for k in range(top_count):
        route_weight = jnp.where(routed_by[k], choice_weight[k][None, :], route_weight)
    weight_high = lax.reduce_precision(route_weight, 8, 7)
    weight_low = route_weight - weight_high

    def spread(values):
        wide = jnp.tile(values, (1, parts))[:, None, :]
        return jnp.where(match, wide, 0.0).astype(jnp.bfloat16).reshape(experts * tall, parts * rows_here)

    combine = jnp.concatenate([spread(weight_high), spread(weight_low)], axis=1)
    mixed = lax.dot_general(
        combine,
        jnp.concatenate(returned, axis=0),
        (((0,), (0,)), ((), ())),
        preferred_element_type=jnp.float32,
    )
    mixed = jnp.sum(mixed.reshape(2, parts, rows_here, width), axis=0).astype(jnp.bfloat16)
    return jnp.concatenate([mixed[p] for p in range(parts)], axis=1), z_loss


def solution(mesh):
    in_specs = (
        P(("dp", "expert"), None),
        P(),
        P(("dp", "expert"), None),
        P("expert", "dp", None),
        P("expert", "dp", None),
        P("expert", "dp", None),
    )
    out_specs = (P(("dp", "expert"), None), P())
    return jax.shard_map(
        on_device, mesh=mesh, in_specs=in_specs, out_specs=out_specs, check_vma=False
    )
```
